32 devices in a mesh: groups: 2 (over x), seq: 16 (over z, y, core).
Axes of the slice: x: 2, y: 2, z: 4, core: 2. Of those that a mesh axis runs over, the one named last changes fastest.
Arguments:
- lengths: int32 [24], P('groups'), parts along dimension 0, may hold values from 1 to 4, as said below
- query: bfloat16 [4096, 4096], P(('groups', 'seq')), parts along dimension 0
- keys: bfloat16 [4096, 1024], P(('groups', 'seq')), parts along dimension 0
- values: bfloat16 [4096, 1024], P(('groups', 'seq')), parts along dimension 0, may hold values from -6 to 6
- new_query: bfloat16 [24, 4096], P('groups'), parts along dimension 0
- new_key: bfloat16 [24, 1024], P('groups'), parts along dimension 0
- new_value: bfloat16 [24, 1024], P('groups'), parts along dimension 0, may hold values from -6 to 6
Outputs:
- prefill: bfloat16 [4096, 4096], P(('groups', 'seq')), parts along dimension 0
- decoded: bfloat16 [24, 4096], P('groups'), parts along dimension 0
The draws below stay inside these ranges and needn't reach their ends.
There are 2 independent parts, one for each index of `groups`. The reference program is written for one: setup_inputs(seed, part) draws one part's arguments, and reference() takes and returns one part's arrays. A program takes and returns all parts, laid end to end along the dimension named above; each array names one. Nothing has to cross between parts.
Inputs may be any that keep to these rules, and one draw needn't show every extreme that they name: Each prompt covers 1 to 4 whole devices, the lengths sum to 16, and one prompt covers exactly 4.
All inputs are finite; a program needn't handle non-finite values.
Results may differ from the reference program's by a relative error of at most 0.0075.
Values may be sent and summed in bfloat16 or wider, within the bound.
A program may use at most 128 MiB of HBM per device.

```python
import jax
import jax.numpy as jnp
from jax import lax

HEADS = 32
KV_HEADS = 8
HEAD_DIM = 128
TOK_DEV = 128
PROMPTS = 12
SPAN_MOST = 4
TOKENS = 2048
N_SEQ = 16


def span_lengths(key):
    base = jax.random.fold_in(key, 11)
    longest = jax.random.randint(jax.random.fold_in(base, 1), (), 0, PROMPTS)
    spare = SPAN_MOST - 1
    devices = TOKENS // TOK_DEV
    extra = devices - SPAN_MOST - (PROMPTS - 1)
    shuffled = jax.random.permutation(jax.random.fold_in(base, 2), (PROMPTS - 1) * spare)
    owners = shuffled[:extra] // spare
    counts = jnp.sum((owners[:, None] == jnp.arange(PROMPTS - 1)[None, :]).astype(jnp.int32), axis=0)
    slots = jnp.arange(PROMPTS)
    others = jnp.clip(jnp.where(slots < longest, slots, slots - 1), 0, PROMPTS - 2)
    return jnp.where(slots == longest, SPAN_MOST, 1 + jnp.take(counts, others)).astype(jnp.int32)


def query_keys(key):
    keys = jnp.clip(jax.random.normal(jax.random.fold_in(key, 21), (TOKENS, KV_HEADS, HEAD_DIM), jnp.float32), -4.0, 4.0)
    query = jnp.clip(jax.random.normal(jax.random.fold_in(key, 22), (TOKENS, HEADS, HEAD_DIM), jnp.float32), -4.0, 4.0)
    new_query = jnp.clip(jax.random.normal(jax.random.fold_in(key, 23), (PROMPTS, HEADS, HEAD_DIM), jnp.float32), -4.0, 4.0)
    new_key = jnp.clip(jax.random.normal(jax.random.fold_in(key, 24), (PROMPTS, KV_HEADS, HEAD_DIM), jnp.float32), -4.0, 4.0)
    return (query, keys, new_query, new_key)


def draw_lengths(key, part):
    return span_lengths(key)


def draw_query(key, part):
    return query_keys(key)[0].reshape(TOKENS, HEADS * HEAD_DIM).astype(jnp.bfloat16)


def draw_keys(key, part):
    return query_keys(key)[1].reshape(TOKENS, KV_HEADS * HEAD_DIM).astype(jnp.bfloat16)


def draw_new_query(key, part):
    return query_keys(key)[2].reshape(PROMPTS, HEADS * HEAD_DIM).astype(jnp.bfloat16)


def draw_new_key(key, part):
    return query_keys(key)[3].reshape(PROMPTS, KV_HEADS * HEAD_DIM).astype(jnp.bfloat16)


def levels(stream_key, shape, shards, smallest, largest):
    def one(position, shards_of):
        heights = jax.random.uniform(jax.random.fold_in(jax.random.fold_in(stream_key, 6), position), (shards_of,), jnp.float32, smallest / len(shards), largest / len(shards))
        return jnp.repeat(jnp.exp(heights), shape[position] // shards_of).reshape((-1,) + (1,) * (len(shape) - position - 1))

    level = one(*shards[0])
    for cut in shards[1:]:
        level = level * one(*cut)
    return level


def scatter_about(stream_key, shape, spread, reach, shards=(), kind=jnp.bfloat16):
    values = spread * jax.random.normal(stream_key, shape, jnp.float32)
    if shards:
        values = values * levels(stream_key, shape, shards, -0.22, 0.18)
    return jnp.clip(values, -reach, reach).astype(kind)


def setup_inputs(seed: int = 0, part: int = 0) -> dict:
    key_list = jax.random.split(jax.random.key(seed), 8)
    part_keys = jax.random.split(jax.random.fold_in(key_list[7], part), 8)
    lengths = draw_lengths(jax.random.fold_in(jax.random.fold_in(key_list[7], part), 71), part)
    query = draw_query(jax.random.fold_in(jax.random.fold_in(key_list[7], part), 71), part)
    keys = draw_keys(jax.random.fold_in(jax.random.fold_in(key_list[7], part), 71), part)
    values = scatter_about(part_keys[3], (TOKENS, KV_HEADS * HEAD_DIM), 1.0, 6.0, ((0, 16),))
    new_query = draw_new_query(jax.random.fold_in(jax.random.fold_in(key_list[7], part), 71), part)
    new_key = draw_new_key(jax.random.fold_in(jax.random.fold_in(key_list[7], part), 71), part)
    new_value = scatter_about(part_keys[6], (PROMPTS, KV_HEADS * HEAD_DIM), 1.0, 6.0)
    return {"lengths": lengths, "query": query, "keys": keys, "values": values, "new_query": new_query, "new_key": new_key, "new_value": new_value}


def to_bf16_f32(array):
    return lax.optimization_barrier(array.astype(jnp.bfloat16)).astype(jnp.float32)


def reference(lengths, query, keys, values, new_query, new_key, new_value):
    group = HEADS // KV_HEADS
    scaling = HEAD_DIM ** -0.5
    ends = jnp.cumsum(lengths).astype(jnp.int32)
    starts = (ends - lengths).astype(jnp.int32)
    devices = jnp.arange(N_SEQ, dtype=jnp.int32)
    dev_start = jnp.max(jnp.where(starts[None, :] <= devices[:, None], starts[None, :], 0), axis=1) * TOK_DEV
    window = SPAN_MOST * TOK_DEV
    padding = (SPAN_MOST - 1) * TOK_DEV
    key_pad = jnp.concatenate([jnp.zeros((padding, KV_HEADS * HEAD_DIM), jnp.bfloat16), keys], axis=0)
    value_pad = jnp.concatenate([jnp.zeros((padding, KV_HEADS * HEAD_DIM), jnp.bfloat16), values], axis=0)

    def one_block(index):
        index = index.astype(jnp.int32)
        q_block = lax.dynamic_slice_in_dim(query, index * TOK_DEV, TOK_DEV, 0).astype(jnp.float32)
        k_block = lax.dynamic_slice_in_dim(key_pad, index * TOK_DEV, window, 0).astype(jnp.float32)
        v_block = lax.dynamic_slice_in_dim(value_pad, index * TOK_DEV, window, 0).astype(jnp.float32)
        q_block = q_block.reshape(TOK_DEV, KV_HEADS, group, HEAD_DIM)
        k_block = k_block.reshape(window, KV_HEADS, HEAD_DIM)
        v_block = v_block.reshape(window, KV_HEADS, HEAD_DIM)
        q_pos = index * TOK_DEV + jnp.arange(TOK_DEV, dtype=jnp.int32)
        k_pos = (index - SPAN_MOST + 1) * TOK_DEV + jnp.arange(window, dtype=jnp.int32)
        start_tok = dev_start[index]
        scores = jnp.einsum('qngd,knd->ngqk', q_block, k_block, precision=lax.Precision.HIGHEST) * scaling
        allowed = (k_pos[None, :] <= q_pos[:, None]) & (k_pos[None, :] >= start_tok)
        scores = jnp.where(allowed, scores, -1e30)
        peak = jnp.max(scores, axis=-1)
        weights = jnp.where(allowed, jnp.exp(scores - peak[..., None]), 0.0)
        total = jnp.sum(weights, axis=-1)
        result = jnp.einsum('ngqk,knd->qngd', to_bf16_f32(weights), v_block, precision=lax.Precision.HIGHEST)
        result = result / jnp.transpose(total, (2, 0, 1))[..., None]
        return result.reshape(TOK_DEV, HEADS * HEAD_DIM).astype(jnp.bfloat16)

    prefill = lax.map(one_block, jnp.arange(N_SEQ, dtype=jnp.int32)).reshape(TOKENS, HEADS * HEAD_DIM)

    tok_device = jnp.arange(TOKENS, dtype=jnp.int32) // TOK_DEV
    member = (tok_device[None, :] >= starts[:, None]) & (tok_device[None, :] < ends[:, None])
    new_q = new_query.astype(jnp.float32).reshape(PROMPTS, KV_HEADS, group, HEAD_DIM)
    new_k = new_key.astype(jnp.float32).reshape(PROMPTS, KV_HEADS, HEAD_DIM)
    new_v = new_value.astype(jnp.float32).reshape(PROMPTS, KV_HEADS, HEAD_DIM)
    all_k = keys.astype(jnp.float32).reshape(TOKENS, KV_HEADS, HEAD_DIM)
    all_v = values.astype(jnp.float32).reshape(TOKENS, KV_HEADS, HEAD_DIM)
    dscores = jnp.einsum('pngd,tnd->ngpt', new_q, all_k, precision=lax.Precision.HIGHEST) * scaling
    own_score = jnp.einsum('pngd,pnd->ngp', new_q, new_k, precision=lax.Precision.HIGHEST) * scaling
    mask = member[None, None, :, :]
    dpeak = jnp.maximum(jnp.max(jnp.where(mask, dscores, -1e30), axis=-1), own_score)
    dweights = jnp.where(mask, jnp.exp(dscores - dpeak[..., None]), 0.0)
    own_weight = jnp.exp(own_score - dpeak)
    dtotal = jnp.sum(dweights, axis=-1) + own_weight
    accum = jnp.einsum('ngpt,tnd->pngd', to_bf16_f32(dweights), all_v, precision=lax.Precision.HIGHEST)
    accum = accum + jnp.transpose(to_bf16_f32(own_weight), (2, 0, 1))[..., None] * new_v[:, :, None, :]
    decoded = accum / jnp.transpose(dtotal, (2, 0, 1))[..., None]
    return prefill, decoded.reshape(PROMPTS, HEADS * HEAD_DIM).astype(jnp.bfloat16)
```

```python
import functools
import math

import jax
import jax.numpy as jnp
from jax import lax
from jax.experimental import pallas as pl
from jax.experimental.pallas import tpu as pltpu
from jax.sharding import PartitionSpec as P

HEAD_DIM = 128
LOW = -1e30
HIGH = 3e38
AHEAD = 3


def body(lengths, query, keys, values, new_query, new_key, new_value):
    n_seq = lax.axis_size("seq")
    reach = n_seq // 4
    half = reach // 2
    tok = query.shape[0]
    hd = HEAD_DIM
    heads = query.shape[1] // hd
    kvh = keys.shape[1] // hd
    group = heads // kvh
    prompts = new_query.shape[0]
    span = reach * tok
    coef = math.log2(math.e) / math.sqrt(hd)
    quads = n_seq // 4
    f32, bf16 = jnp.float32, jnp.bfloat16

    def kernel(len_ref, q_hbm, k_hbm, v_hbm, nq_ref, nk_ref, nv_ref, out_hbm, dec_ref,
               qbuf, kvb, obuf, dbuf, qd, nk32, nv32, oall, tri,
               load_sem, q_sem, out_sem, send_sem, fwd_sem, recv_sem, d_send, d_recv):
        me = lax.axis_index("seq")
        core = lax.rem(me, 2)
        sibling = me + 1 - 2 * core

        def load_copies(h):
            return [
                pltpu.make_async_copy(
                    src.at[:, pl.ds(h * hd, hd)],
                    kvb.at[h, part, pl.ds((reach - 1) * tok, tok), :],
                    load_sem.at[h, part],
                )
                for part, src in enumerate((k_hbm, v_hbm))
            ]

        for h in range(kvh):
            for copy in load_copies(h):
                copy.start()
        q_copy = pltpu.make_async_copy(q_hbm, qbuf, q_sem)
        q_copy.start()

        barrier = pltpu.get_barrier_semaphore()
        for k in range(1, n_seq):
            pl.semaphore_signal(barrier, inc=1, device_id={"seq": lax.rem(me + k, n_seq)},
                                device_id_type=pl.DeviceIdType.MESH)

        run = jnp.int32(0)
        first_dev, pid, is_last = jnp.int32(0), jnp.int32(0), jnp.int32(0)
        starts, sizes = [], []
        for p in range(prompts):
            size = len_ref[p]
            starts.append(run)
            sizes.append(size)
            inside = (run <= me) & (me < run + size)
            first_dev = jnp.where(inside, run, first_dev)
            pid = jnp.where(inside, p, pid)
            is_last = jnp.where(inside & (me == run + size - 1), 1, is_last)
            run = run + size

        rows = lax.broadcasted_iota(jnp.int32, (tok, tok), 0)
        cols = lax.broadcasted_iota(jnp.int32, (tok, tok), 1)
        tri[...] = jnp.where(cols <= rows, HIGH, LOW)

        def slot(d):
            return pl.ds((reach - 1 - d) * tok, tok)

        for d in range(1, reach):
            @pl.when(me < d)
            def _(d=d):
                kvb[:, :, slot(d), :] = jnp.zeros((kvh, 2, tok, hd), bf16)

        for h in range(kvh):
            for copy in load_copies(h):
                copy.wait()
        pl.semaphore_wait(barrier, n_seq - 1)

        def remote(h, held, put, sem, target):
            return pltpu.make_async_remote_copy(
                src_ref=kvb.at[h, :, pl.ds(held * tok, tok), :],
                dst_ref=kvb.at[h, :, pl.ds(put * tok, tok), :],
                send_sem=sem,
                recv_sem=recv_sem.at[h, put],
                device_id={"seq": target},
                device_id_type=pl.DeviceIdType.MESH,
            )

        own = reach - 1

        def each_send(h, act):
            @pl.when(core == 0)
            def _():
                act(remote(h, own, reach - 2, send_sem.at[h, half - 1], me + 1))
            for j in range(1, half):
                @pl.when(me + 2 * j < n_seq)
                def _(j=j):
                    act(remote(h, own, own - 2 * j, send_sem.at[h, j - 1], me + 2 * j))
            @pl.when((core == 1) & (me + reach - 1 < n_seq))
            def _():
                act(remote(h, own, 0, send_sem.at[h, half - 1], me + reach - 1))

        def each_forward(h, act, arrive):
            for j in range(1, half):
                @pl.when(me >= 2 * j)
                def _(j=j):
                    put = own - 2 * j - 1 + 2 * core
                    copy = remote(h, own - 2 * j, put, fwd_sem.at[h, j - 1], sibling)
                    if arrive:
                        remote(h, own, own - 2 * j, fwd_sem.at[h, j - 1], sibling).wait_recv()
                    act(copy)

        def wait_rest(h):
            for j in range(half):
                @pl.when(me >= 2 * j + 1)
                def _(j=j):
                    remote(h, own, own - 2 * j - 1, fwd_sem.at[h, 0], sibling).wait_recv()

        start = lambda c: c.start()
        wait_send = lambda c: c.wait_send()
        for h in range(min(AHEAD, kvh)):
            each_send(h, start)

        picked = lax.broadcasted_iota(jnp.int32, (prompts, hd), 0) == pid

        def pick(ref, h):
            block = ref[:, h * hd:(h + 1) * hd].astype(f32)
            return jnp.sum(jnp.where(picked, block, 0.0), axis=0, keepdims=True)

        for h in range(heads):
            qd[h:h + 1, :] = pick(nq_ref, h)
        for h in range(kvh):
            nk32[h * group:(h + 1) * group, :] = jnp.broadcast_to(pick(nk_ref, h), (group, hd))
            nv32[h * group:(h + 1) * group, :] = jnp.broadcast_to(pick(nv_ref, h), (group, hd))
        q32 = qd[...]
        q32b = q32.astype(bf16)
        row_head = lax.broadcasted_iota(jnp.int32, (heads, tok), 0) // group
        own_rows = pl.ds((reach - 1) * tok, tok)
        contract_last = (((1,), (1,)), ((), ()))
        scores = jnp.zeros((heads, tok), f32)
        for h in range(kvh):
            part = lax.dot_general(q32b, kvb[h, 0, own_rows, :], contract_last,
                                   preferred_element_type=f32)
            scores = jnp.where(row_head == h, part, scores)
        own_score = jnp.sum(q32 * nk32[...], axis=1, keepdims=True)
        own_score = jnp.where(is_last == 1, own_score, LOW)
        peak = jnp.maximum(jnp.max(scores, axis=1, keepdims=True), own_score)
        weights = jnp.exp2((scores - peak) * coef)
        own_weight = jnp.exp2((own_score - peak) * coef)
        total = jnp.sum(weights, axis=1, keepdims=True) + own_weight
        accum = own_weight.astype(bf16).astype(f32) * nv32[...]
        for h in range(kvh):
            masked = jnp.where(row_head == h, weights, 0.0).astype(bf16)
            accum += jnp.dot(masked, kvb[h, 1, own_rows, :], preferred_element_type=f32)

        quad = me // 4
        side = lax.rem(me // 2, 2)
        dbuf[quad, core, side, 0:heads, :] = accum / total
        dbuf[quad, core, side, heads:, :] = jnp.broadcast_to(
            peak * coef + jnp.log2(total), (heads, hd))

        def d_copy(ref, send, recv, target):
            return pltpu.make_async_remote_copy(
                src_ref=ref, dst_ref=ref, send_sem=d_send.at[send], recv_sem=d_recv.at[recv],
                device_id={"seq": target}, device_id_type=pl.DeviceIdType.MESH)

        across = me + 2 - 4 * side
        d_first = d_copy(dbuf.at[quad, core, side], 0, 0, across)
        d_first_in = d_copy(dbuf.at[quad, core, 1 - side], 0, 0, across)
        d_far = [d_copy(dbuf.at[quad, core], k, k, lax.rem(me + 4 * k, n_seq))
                 for k in range(1, quads)]
        d_far_in = [d_copy(dbuf.at[lax.rem(quad + quads - k, quads), core], k, k, sibling)
                    for k in range(1, quads)]
        d_last = d_copy(dbuf.at[:, core], quads, quads, sibling)
        d_last_in = d_copy(dbuf.at[:, 1 - core], quads, quads, sibling)

        d_first.start()
        q_copy.wait()

        block_of = lax.broadcasted_iota(jnp.int32, (1, span - tok), 1) // tok
        cap = jnp.where(me - (reach - 1) + block_of >= first_dev, HIGH, LOW)

        def out_copy(h):
            at = pl.ds(pl.multiple_of(h * group * hd, hd), group * hd)
            return pltpu.make_async_copy(obuf.at[:, at], out_hbm.at[:, at], out_sem.at[h])

        def attend(h):
            k_all = kvb[h, 0]
            v_all = kvb[h, 1]
            for g in range(group):
                at = pl.ds(pl.multiple_of((h * group + g) * hd, hd), hd)
                s = lax.dot_general(qbuf[:, at], k_all, contract_last,
                                    preferred_element_type=f32)
                far = jnp.minimum(s[:, :span - tok], cap)
                near = jnp.minimum(s[:, span - tok:], tri[...])
                top = jnp.maximum(jnp.max(far, axis=1, keepdims=True),
                                  jnp.max(near, axis=1, keepdims=True))
                w = jnp.exp2((jnp.concatenate([far, near], axis=1) - top) * coef)
                tot = jnp.sum(w, axis=1, keepdims=True)
                o = jnp.dot(w.astype(bf16), v_all, preferred_element_type=f32)
                obuf[:, at] = (o * (1.0 / tot)).astype(bf16)
            out_copy(h).start()

        def combine():
            d_last_in.wait_recv()
            for p in range(prompts):
                parts = []
                for k in range(reach):
                    d = jnp.minimum(starts[p] + k, n_seq - 1)
                    a, b, c = d // 4, lax.rem(d, 2), lax.rem(d // 2, 2)
                    lse = jnp.where(k < sizes[p], dbuf[a, b, c, heads:, :], LOW)
                    parts.append((lse, a, b, c))
                m = functools.reduce(jnp.maximum, [x[0] for x in parts])
                num = jnp.zeros((heads, hd), f32)
                den = jnp.zeros((heads, hd), f32)
                for lse, a, b, c in parts:
                    w = jnp.exp2(lse - m)
                    den += w
                    num += w * dbuf[a, b, c, 0:heads, :]
                oall[p * heads:(p + 1) * heads, :] = num / den
            for h in range(heads):
                dec_ref[:, h * hd:(h + 1) * hd] = oall[
                    pl.ds(h, prompts, stride=heads), :].astype(bf16)

        far_at = min(2, kvh - 1)
        last_at = min(5, kvh - 1)

        def step(h, carry):
            @pl.when(h + AHEAD < kvh)
            def _():
                each_send(h + AHEAD, start)

            @pl.when(h == far_at)
            def _():
                d_first_in.wait_recv()
                for c in d_far:
                    c.start()

            @pl.when(h == last_at)
            def _():
                for c in d_far_in:
                    c.wait_recv()
                d_last.start()

            @pl.when(h == kvh - 1)
            def _():
                combine()

            each_forward(h, start, True)

            @pl.when(h >= 1)
            def _():
                wait_rest(h - 1)
                attend(h - 1)
            return carry

        lax.fori_loop(0, kvh, step, 0)
        wait_rest(kvh - 1)
        attend(kvh - 1)

        d_first.wait_send()
        for c in d_far:
            c.wait_send()
        d_last.wait_send()

        def drain(h, carry):
            each_send(h, wait_send)
            each_forward(h, wait_send, False)
            out_copy(h).wait()
            return carry

        lax.fori_loop(0, kvh, drain, 0)

    any_spec = pl.BlockSpec(memory_space=pl.ANY)
    vmem = pl.BlockSpec(memory_space=pltpu.VMEM)
    return pl.pallas_call(
        kernel,
        out_shape=(
            jax.ShapeDtypeStruct((tok, heads * hd), bf16),
            jax.ShapeDtypeStruct((prompts, heads * hd), bf16),
        ),
        in_specs=[pl.BlockSpec(memory_space=pltpu.SMEM)] + [any_spec] * 3 + [vmem] * 3,
        out_specs=(any_spec, vmem),
        scratch_shapes=[
            pltpu.VMEM((tok, heads * hd), bf16),
            pltpu.VMEM((kvh, 2, span, hd), bf16),
            pltpu.VMEM((tok, heads * hd), bf16),
            pltpu.VMEM((quads, 2, 2, 2 * heads, hd), f32),
            pltpu.VMEM((heads, hd), f32),
            pltpu.VMEM((heads, hd), f32),
            pltpu.VMEM((heads, hd), f32),
            pltpu.VMEM((prompts * heads, hd), f32),
            pltpu.VMEM((tok, tok), f32),
            pltpu.SemaphoreType.DMA((kvh, 2)),
            pltpu.SemaphoreType.DMA,
            pltpu.SemaphoreType.DMA((kvh,)),
            pltpu.SemaphoreType.DMA((kvh, half)),
            pltpu.SemaphoreType.DMA((kvh, half)),
            pltpu.SemaphoreType.DMA((kvh, reach)),
            pltpu.SemaphoreType.DMA((quads + 1,)),
            pltpu.SemaphoreType.DMA((quads + 1,)),
        ],
        compiler_params=pltpu.CompilerParams(
            collective_id=0, has_side_effects=True, vmem_limit_bytes=56 * 1024 * 1024
        ),
    )(lengths, query, keys, values, new_query, new_key, new_value)


def solution(mesh):
    in_specs = (
        P("groups"),
        P(("groups", "seq"), None),
        P(("groups", "seq"), None),
        P(("groups", "seq"), None),
        P("groups", None),
        P("groups", None),
        P("groups", None),
    )
    out_specs = (P(("groups", "seq"), None), P("groups", None))
    return jax.shard_map(body, mesh=mesh, in_specs=in_specs, out_specs=out_specs, check_vma=False)
```

```python
import functools
import math

import jax
import jax.numpy as jnp
from jax import lax
from jax.experimental import pallas as pl
from jax.experimental.pallas import tpu as pltpu
from jax.sharding import PartitionSpec as P

HEAD_DIM = 128
LOW = -1e30
HIGH = 3e38
AHEAD = 3
LEAD = 2


def body(lengths, query, keys, values, new_query, new_key, new_value):
    n_seq = lax.axis_size("seq")
    reach = n_seq // 4
    half = reach // 2
    tok = query.shape[0]
    hd = HEAD_DIM
    heads = query.shape[1] // hd
    kvh = keys.shape[1] // hd
    group = heads // kvh
    prompts = new_query.shape[0]
    span = reach * tok
    coef = math.log2(math.e) / math.sqrt(hd)
    quads = n_seq // 4
    f32, bf16 = jnp.float32, jnp.bfloat16

    def kernel(len_ref, q_hbm, k_hbm, v_hbm, nq_ref, nk_ref, nv_ref, out_ref, dec_ref,
               qbuf, kvb, dbuf, qd, nk32, nv32, oall, lall, tri,
               load_sem, q_sem, send_sem, fwd_sem, relay_sem, recv_sem, d_send, d_recv):
        me = lax.axis_index("seq")
        core = lax.rem(me, 2)
        sibling = me + 1 - 2 * core

        def load_copies(h):
            return [
                pltpu.make_async_copy(
                    src.at[:, pl.ds(h * hd, hd)],
                    kvb.at[h, part, pl.ds((reach - 1) * tok, tok), :],
                    load_sem.at[h, part],
                )
                for part, src in enumerate((k_hbm, v_hbm))
            ]

        for h in range(kvh):
            for copy in load_copies(h):
                copy.start()
        q_copy = pltpu.make_async_copy(q_hbm, qbuf, q_sem)
        q_copy.start()

        barrier = pltpu.get_barrier_semaphore()
        for k in range(1, n_seq):
            pl.semaphore_signal(barrier, inc=1, device_id={"seq": lax.rem(me + k, n_seq)},
                                device_id_type=pl.DeviceIdType.MESH)

        run = jnp.int32(0)
        first_dev, pid, is_last = jnp.int32(0), jnp.int32(0), jnp.int32(0)
        starts, sizes = [], []
        for p in range(prompts):
            size = len_ref[p]
            starts.append(run)
            sizes.append(size)
            inside = (run <= me) & (me < run + size)
            first_dev = jnp.where(inside, run, first_dev)
            pid = jnp.where(inside, p, pid)
            is_last = jnp.where(inside & (me == run + size - 1), 1, is_last)
            run = run + size

        rows = lax.broadcasted_iota(jnp.int32, (tok, tok), 0)
        cols = lax.broadcasted_iota(jnp.int32, (tok, tok), 1)
        tri[...] = jnp.where(cols <= rows, HIGH, LOW)

        def slot(d):
            return pl.ds((reach - 1 - d) * tok, tok)

        for d in range(1, reach):
            @pl.when(me < d)
            def _(d=d):
                kvb[:, :, slot(d), :] = jnp.zeros((kvh, 2, tok, hd), bf16)

        for h in range(kvh):
            for copy in load_copies(h):
                copy.wait()
        pl.semaphore_wait(barrier, n_seq - 1)

        def remote(h, held, put, sem, target):
            return pltpu.make_async_remote_copy(
                src_ref=kvb.at[h, :, pl.ds(held * tok, tok), :],
                dst_ref=kvb.at[h, :, pl.ds(put * tok, tok), :],
                send_sem=sem,
                recv_sem=recv_sem.at[h, put],
                device_id={"seq": target},
                device_id_type=pl.DeviceIdType.MESH,
            )

        own = reach - 1

        odd = lax.rem(me // 2, 2)
        relayed = (core == 1) & (odd == 1) if half == 2 else (core == 2)
        relays = (core == 0) & (odd == 1) & (me >= reach - 1) if half == 2 else (core == 2)

        def each_near(h, act):
            @pl.when(core == 0)
            def _():
                act(remote(h, own, reach - 2, send_sem.at[h, half - 1], me + 1))
            @pl.when((core == 1) & (me + reach - 1 < n_seq))
            def _():
                act(remote(h, own, 0, send_sem.at[h, half - 1], me + reach - 1))

        def each_send(h, act):
            for j in range(1, half):
                @pl.when((me + 2 * j < n_seq) & jnp.logical_not(relayed))
                def _(j=j):
                    act(remote(h, own, own - 2 * j, send_sem.at[h, j - 1], me + 2 * j))

        def each_relay(h, act, arrive):
            if half == 2:
                @pl.when(relays)
                def _():
                    if arrive:
                        remote(h, own, 0, relay_sem.at[h], sibling).wait_recv()
                    act(remote(h, 0, own - 2, relay_sem.at[h], me - 1))

        def each_forward(h, act, arrive):
            for j in range(1, half):
                @pl.when(me >= 2 * j)
                def _(j=j):
                    put = own - 2 * j - 1 + 2 * core
                    copy = remote(h, own - 2 * j, put, fwd_sem.at[h, j - 1], sibling)
                    if arrive:
                        remote(h, own, own - 2 * j, fwd_sem.at[h, j - 1], sibling).wait_recv()
                    act(copy)

        def wait_rest(h):
            for j in range(half):
                here = me >= 2 * j + 1
                if j == half - 1:
                    here = here & jnp.logical_not(relays)
                @pl.when(here)
                def _(j=j):
                    remote(h, own, own - 2 * j - 1, fwd_sem.at[h, 0], sibling).wait_recv()

        start = lambda c: c.start()
        wait_send = lambda c: c.wait_send()
        for h in range(kvh):
            each_near(h, start)
            if h < AHEAD:
                each_send(h, start)

        picked = lax.broadcasted_iota(jnp.int32, (prompts, hd), 0) == pid

        def pick(ref, h):
            block = ref[:, h * hd:(h + 1) * hd].astype(f32)
            return jnp.sum(jnp.where(picked, block, 0.0), axis=0, keepdims=True)

        for h in range(heads):
            qd[h:h + 1, :] = pick(nq_ref, h)
        for h in range(kvh):
            nk32[h * group:(h + 1) * group, :] = jnp.broadcast_to(pick(nk_ref, h), (group, hd))
            nv32[h * group:(h + 1) * group, :] = jnp.broadcast_to(pick(nv_ref, h), (group, hd))
        q32 = qd[...]
        q32b = q32.astype(bf16)
        row_head = lax.broadcasted_iota(jnp.int32, (heads, tok), 0) // group
        own_rows = pl.ds((reach - 1) * tok, tok)
        contract_last = (((1,), (1,)), ((), ()))
        scores = jnp.zeros((heads, tok), f32)
        for h in range(kvh):
            part = lax.dot_general(q32b, kvb[h, 0, own_rows, :], contract_last,
                                   preferred_element_type=f32)
            scores = jnp.where(row_head == h, part, scores)
        own_score = jnp.sum(q32 * nk32[...], axis=1, keepdims=True)
        own_score = jnp.where(is_last == 1, own_score, LOW)
        peak = jnp.maximum(jnp.max(scores, axis=1, keepdims=True), own_score)
        weights = jnp.exp2((scores - peak) * coef)
        own_weight = jnp.exp2((own_score - peak) * coef)
        total = jnp.sum(weights, axis=1, keepdims=True) + own_weight
        accum = own_weight.astype(bf16).astype(f32) * nv32[...]
        for h in range(kvh):
            masked = jnp.where(row_head == h, weights, 0.0).astype(bf16)
            accum += jnp.dot(masked, kvb[h, 1, own_rows, :], preferred_element_type=f32)

        quad = me // 4
        side = lax.rem(me // 2, 2)
        dbuf[quad, core, side, 0:heads, :] = accum / total
        diag = (lax.broadcasted_iota(jnp.int32, (heads, hd), 0)
                == lax.broadcasted_iota(jnp.int32, (heads, hd), 1))
        level = jnp.where(diag, peak * coef + jnp.log2(total), 0.0)
        dbuf[quad, core, side, heads:, :] = jnp.broadcast_to(
            jnp.sum(level, axis=0, keepdims=True), (8, hd))

        def d_copy(ref, send, recv, target):
            return pltpu.make_async_remote_copy(
                src_ref=ref, dst_ref=ref, send_sem=d_send.at[send], recv_sem=d_recv.at[recv],
                device_id={"seq": target}, device_id_type=pl.DeviceIdType.MESH)

        across = me + 2 - 4 * side
        d_first = d_copy(dbuf.at[quad, core, side], 0, 0, across)
        d_first_in = d_copy(dbuf.at[quad, core, 1 - side], 0, 0, across)
        d_far = [d_copy(dbuf.at[quad, core], k, k, lax.rem(me + 4 * k, n_seq))
                 for k in range(1, quads)]
        d_far_in = [d_copy(dbuf.at[lax.rem(quad + quads - k, quads), core], k, k, sibling)
                    for k in range(1, quads)]
        d_last = d_copy(dbuf.at[:, core], quads, quads, sibling)
        d_last_in = d_copy(dbuf.at[:, 1 - core], quads, quads, sibling)

        d_first.start()
        q_copy.wait()

        block_of = lax.broadcasted_iota(jnp.int32, (1, span - tok), 1) // tok
        cap = jnp.where(me - (reach - 1) + block_of >= first_dev, HIGH, LOW)

        def attend(h):
            k_all = kvb[h, 0]
            v_all = kvb[h, 1]
            for g in range(group):
                at = pl.ds(pl.multiple_of((h * group + g) * hd, hd), hd)
                s = lax.dot_general(qbuf[:, at], k_all, contract_last,
                                    preferred_element_type=f32)
                far = jnp.minimum(s[:, :span - tok], cap)
                near = jnp.minimum(s[:, span - tok:], tri[...])
                top = jnp.maximum(jnp.max(far, axis=1, keepdims=True),
                                  jnp.max(near, axis=1, keepdims=True))
                w = jnp.exp2((jnp.concatenate([far, near], axis=1) - top) * coef)
                tot = jnp.sum(w, axis=1, keepdims=True)
                o = jnp.dot(w.astype(bf16), v_all, preferred_element_type=f32)
                out_ref[:, at] = (o * (1.0 / tot)).astype(bf16)

        def combine():
            d_last_in.wait_recv()
            for d in range(n_seq):
                level = jnp.where(diag, dbuf[d // 4, d % 2, d // 2 % 2, heads:heads + 1, :], 0.0)
                lall[d] = jnp.broadcast_to(jnp.sum(level, axis=1, keepdims=True), (heads, hd))
            for p in range(prompts):
                parts = []
                for k in range(reach):
                    d = jnp.minimum(starts[p] + k, n_seq - 1)
                    a, b, c = d // 4, lax.rem(d, 2), lax.rem(d // 2, 2)
                    lse = jnp.where(k < sizes[p], lall[d], LOW)
                    parts.append((lse, a, b, c))
                m = functools.reduce(jnp.maximum, [x[0] for x in parts])
                num = jnp.zeros((heads, hd), f32)
                den = jnp.zeros((heads, hd), f32)
                for lse, a, b, c in parts:
                    w = jnp.exp2(lse - m)
                    den += w
                    num += w * dbuf[a, b, c, 0:heads, :]
                oall[p * heads:(p + 1) * heads, :] = num / den
            for h in range(heads):
                dec_ref[:, h * hd:(h + 1) * hd] = oall[
                    pl.ds(h, prompts, stride=heads), :].astype(bf16)

        far_at = min(2, kvh - 1)
        last_at = min(5, kvh - 1)

        def step(h, carry):
            @pl.when(h + AHEAD < kvh)
            def _():
                each_send(h + AHEAD, start)

            @pl.when(h == far_at)
            def _():
                d_first_in.wait_recv()
                for c in d_far:
                    c.start()

            @pl.when(h == last_at)
            def _():
                for c in d_far_in:
                    c.wait_recv()
                d_last.start()

            @pl.when(h == kvh - 1)
            def _():
                combine()

            @pl.when(h + LEAD < kvh)
            def _():
                each_relay(h + LEAD, start, True)

            each_forward(h, start, True)

            @pl.when(h >= 1)
            def _():
                wait_rest(h - 1)
                attend(h - 1)
            return carry

        for h in range(min(LEAD, kvh)):
            each_relay(h, start, True)
        lax.fori_loop(0, kvh, step, 0)
        wait_rest(kvh - 1)
        attend(kvh - 1)

        d_first.wait_send()
        for c in d_far:
            c.wait_send()
        d_last.wait_send()

        def drain(h, carry):
            each_send(h, wait_send)
            each_near(h, wait_send)
            each_forward(h, wait_send, False)
            each_relay(h, wait_send, False)
            return carry

        lax.fori_loop(0, kvh, drain, 0)

    any_spec = pl.BlockSpec(memory_space=pl.ANY)
    vmem = pl.BlockSpec(memory_space=pltpu.VMEM)
    return pl.pallas_call(
        kernel,
        out_shape=(
            pltpu.VMEM((tok, heads * hd), bf16),
            pltpu.VMEM((prompts, heads * hd), bf16),
        ),
        in_specs=[pl.BlockSpec(memory_space=pltpu.SMEM)] + [any_spec] * 3 + [vmem] * 3,
        out_specs=(vmem, vmem),
        scratch_shapes=[
            pltpu.VMEM((tok, heads * hd), bf16),
            pltpu.VMEM((kvh, 2, span, hd), bf16),
            pltpu.VMEM((quads, 2, 2, heads + 8, hd), f32),
            pltpu.VMEM((heads, hd), f32),
            pltpu.VMEM((heads, hd), f32),
            pltpu.VMEM((heads, hd), f32),
            pltpu.VMEM((prompts * heads, hd), f32),
            pltpu.VMEM((n_seq, heads, hd), f32),
            pltpu.VMEM((tok, tok), f32),
            pltpu.SemaphoreType.DMA((kvh, 2)),
            pltpu.SemaphoreType.DMA,
            pltpu.SemaphoreType.DMA((kvh, half)),
            pltpu.SemaphoreType.DMA((kvh, half)),
            pltpu.SemaphoreType.DMA((kvh,)),
            pltpu.SemaphoreType.DMA((kvh, reach)),
            pltpu.SemaphoreType.DMA((quads + 1,)),
            pltpu.SemaphoreType.DMA((quads + 1,)),
        ],
        compiler_params=pltpu.CompilerParams(
            collective_id=0, has_side_effects=True, vmem_limit_bytes=56 * 1024 * 1024
        ),
    )(lengths, query, keys, values, new_query, new_key, new_value)


def solution(mesh):
    in_specs = (
        P("groups"),
        P(("groups", "seq"), None),
        P(("groups", "seq"), None),
        P(("groups", "seq"), None),
        P("groups", None),
        P("groups", None),
        P("groups", None),
    )
    out_specs = (P(("groups", "seq"), None), P("groups", None))
    return jax.shard_map(body, mesh=mesh, in_specs=in_specs, out_specs=out_specs, check_vma=False)
```

```python
import functools
import math

import jax
import jax.numpy as jnp
from jax import lax
from jax.experimental import pallas as pl
from jax.experimental.pallas import tpu as pltpu
from jax.sharding import PartitionSpec as P

HEAD_DIM = 128
LOW = -1e30
HIGH = 3e38
AHEAD = 3
LEAD = 2
PACK = 2


def body(lengths, query, keys, values, new_query, new_key, new_value):
    n_seq = lax.axis_size("seq")
    reach = n_seq // 4
    half = reach // 2
    tok = query.shape[0]
    hd = HEAD_DIM
    heads = query.shape[1] // hd
    kvh = keys.shape[1] // hd
    group = heads // kvh
    prompts = new_query.shape[0]
    span = reach * tok
    coef = math.log2(math.e) / math.sqrt(hd)
    quads = n_seq // 4
    f32, bf16 = jnp.float32, jnp.bfloat16

    def kernel(len_ref, q_hbm, k_hbm, v_hbm, nq_hbm, nk_hbm, nv_hbm, out_ref, dec_ref,
               nq_ref, nk_ref, nv_ref, qbuf, kvb, dbuf, qd, nk32, nv32, oall, lall, tri,
               load_sem, q_sem, n_sem, send_sem, fwd_sem, relay_sem, recv_sem, d_send, d_recv):
        me = lax.axis_index("seq")
        core = lax.rem(me, 2)
        sibling = me + 1 - 2 * core

        def load_copies(h):
            return [
                pltpu.make_async_copy(
                    src.at[:, pl.ds(h * hd, hd)],
                    kvb.at[h, part, pl.ds((reach - 1) * tok, tok), :],
                    load_sem.at[h, part],
                )
                for part, src in enumerate((k_hbm, v_hbm))
            ]

        for h in range(kvh):
            for copy in load_copies(h):
                copy.start()
        q_copy = pltpu.make_async_copy(q_hbm, qbuf, q_sem)
        n_copies = [pltpu.make_async_copy(src, dst, n_sem.at[n]) for n, (src, dst) in
                    enumerate(((nq_hbm, nq_ref), (nk_hbm, nk_ref), (nv_hbm, nv_ref)))]
        for copy in n_copies:
            copy.start()
        q_copy.start()

        barrier = pltpu.get_barrier_semaphore()
        for k in range(1, n_seq):
            pl.semaphore_signal(barrier, inc=1, device_id={"seq": lax.rem(me + k, n_seq)},
                                device_id_type=pl.DeviceIdType.MESH)

        run = jnp.int32(0)
        first_dev, pid, is_last = jnp.int32(0), jnp.int32(0), jnp.int32(0)
        starts, sizes = [], []
        for p in range(prompts):
            size = len_ref[p]
            starts.append(run)
            sizes.append(size)
            inside = (run <= me) & (me < run + size)
            first_dev = jnp.where(inside, run, first_dev)
            pid = jnp.where(inside, p, pid)
            is_last = jnp.where(inside & (me == run + size - 1), 1, is_last)
            run = run + size

        pl.semaphore_wait(barrier, n_seq - 1)

        def remote(h, held, put, sem, target):
            return pltpu.make_async_remote_copy(
                src_ref=kvb.at[h, :, pl.ds(held * tok, tok), :],
                dst_ref=kvb.at[h, :, pl.ds(put * tok, tok), :],
                send_sem=sem,
                recv_sem=recv_sem.at[h, put],
                device_id={"seq": target},
                device_id_type=pl.DeviceIdType.MESH,
            )

        own = reach - 1

        odd = lax.rem(me // 2, 2)
        relayed = (core == 1) & (odd == 1) if half == 2 else (core == 2)
        relays = (core == 0) & (odd == 1) & (me >= reach - 1) if half == 2 else (core == 2)

        def each_near(h, act):
            @pl.when(core == 0)
            def _():
                act(remote(h, own, reach - 2, send_sem.at[h, half - 1], me + 1))
            @pl.when((core == 1) & (me + reach - 1 < n_seq))
            def _():
                act(remote(h, own, 0, send_sem.at[h, half - 1], me + reach - 1))

        def each_send(h, act):
            for j in range(1, half):
                @pl.when((me + 2 * j < n_seq) & jnp.logical_not(relayed))
                def _(j=j):
                    act(remote(h, own, own - 2 * j, send_sem.at[h, j - 1], me + 2 * j))

        def each_relay(h, act, arrive):
            if half == 2:
                @pl.when(relays)
                def _():
                    if arrive:
                        remote(h, own, 0, relay_sem.at[h], sibling).wait_recv()
                    act(remote(h, 0, own - 2, relay_sem.at[h], me - 1))

        def each_forward(h, act, arrive):
            for j in range(1, half):
                @pl.when(me >= 2 * j)
                def _(j=j):
                    put = own - 2 * j - 1 + 2 * core
                    copy = remote(h, own - 2 * j, put, fwd_sem.at[h, j - 1], sibling)
                    if arrive:
                        remote(h, own, own - 2 * j, fwd_sem.at[h, j - 1], sibling).wait_recv()
                    act(copy)

        def wait_rest(h):
            for j in range(half):
                here = me >= 2 * j + 1
                if j == half - 1:
                    here = here & jnp.logical_not(relays)
                @pl.when(here)
                def _(j=j):
                    remote(h, own, own - 2 * j - 1, fwd_sem.at[h, 0], sibling).wait_recv()

        start = lambda c: c.start()
        wait_send = lambda c: c.wait_send()
        for h in range(kvh):
            for copy in load_copies(h):
                copy.wait()
            each_near(h, start)
            if h < AHEAD:
                each_send(h, start)

        rows = lax.broadcasted_iota(jnp.int32, (tok, tok), 0)
        cols = lax.broadcasted_iota(jnp.int32, (tok, tok), 1)
        tri[...] = jnp.where(cols <= rows, HIGH, LOW)

        def slot(d):
            return pl.ds((reach - 1 - d) * tok, tok)

        for d in range(1, reach):
            @pl.when(me < d)
            def _(d=d):
                kvb[:, :, slot(d), :] = jnp.zeros((kvh, 2, tok, hd), bf16)

        for copy in n_copies:
            copy.wait()
        picked = lax.broadcasted_iota(jnp.int32, (prompts, hd), 0) == pid

        def pick(ref, h):
            block = ref[:, h * hd:(h + 1) * hd].astype(f32)
            return jnp.sum(jnp.where(picked, block, 0.0), axis=0, keepdims=True)

        for h in range(heads):
            qd[h:h + 1, :] = pick(nq_ref, h)
        for h in range(kvh):
            nk32[h * group:(h + 1) * group, :] = jnp.broadcast_to(pick(nk_ref, h), (group, hd))
            nv32[h * group:(h + 1) * group, :] = jnp.broadcast_to(pick(nv_ref, h), (group, hd))
        q32 = qd[...]
        q32b = q32.astype(bf16)
        row_head = lax.broadcasted_iota(jnp.int32, (heads, tok), 0) // group
        own_rows = pl.ds((reach - 1) * tok, tok)
        contract_last = (((1,), (1,)), ((), ()))
        scores = jnp.zeros((heads, tok), f32)
        for h in range(kvh):
            part = lax.dot_general(q32b, kvb[h, 0, own_rows, :], contract_last,
                                   preferred_element_type=f32)
            scores = jnp.where(row_head == h, part, scores)
        own_score = jnp.sum(q32 * nk32[...], axis=1, keepdims=True)
        own_score = jnp.where(is_last == 1, own_score, LOW)
        peak = jnp.maximum(jnp.max(scores, axis=1, keepdims=True), own_score)
        weights = jnp.exp2((scores - peak) * coef)
        own_weight = jnp.exp2((own_score - peak) * coef)
        total = jnp.sum(weights, axis=1, keepdims=True) + own_weight
        accum = own_weight.astype(bf16).astype(f32) * nv32[...]
        for h in range(kvh):
            masked = jnp.where(row_head == h, weights, 0.0).astype(bf16)
            accum += jnp.dot(masked, kvb[h, 1, own_rows, :], preferred_element_type=f32)

        quad = me // 4
        side = lax.rem(me // 2, 2)
        dbuf[quad, core, side, 0:heads, :] = accum / total
        diag = (lax.broadcasted_iota(jnp.int32, (heads, hd), 0)
                == lax.broadcasted_iota(jnp.int32, (heads, hd), 1))
        level = jnp.where(diag, peak * coef + jnp.log2(total), 0.0)
        dbuf[quad, core, side, heads:, :] = jnp.broadcast_to(
            jnp.sum(level, axis=0, keepdims=True), (8, hd))

        def d_copy(ref, send, recv, target):
            return pltpu.make_async_remote_copy(
                src_ref=ref, dst_ref=ref, send_sem=d_send.at[send], recv_sem=d_recv.at[recv],
                device_id={"seq": target}, device_id_type=pl.DeviceIdType.MESH)

        across = me + 2 - 4 * side
        d_first = d_copy(dbuf.at[quad, core, side], 0, 0, across)
        d_first_in = d_copy(dbuf.at[quad, core, 1 - side], 0, 0, across)
        d_far = [d_copy(dbuf.at[quad, core], k, k, lax.rem(me + 4 * k, n_seq))
                 for k in range(1, quads)]
        d_far_in = [d_copy(dbuf.at[lax.rem(quad + quads - k, quads), core], k, k, sibling)
                    for k in range(1, quads)]
        d_last = d_copy(dbuf.at[:, core], quads, quads, sibling)
        d_last_in = d_copy(dbuf.at[:, 1 - core], quads, quads, sibling)

        d_first.start()
        q_copy.wait()

        block_of = lax.broadcasted_iota(jnp.int32, (1, span - tok), 1) // tok
        cap = jnp.where(me - (reach - 1) + block_of >= first_dev, HIGH, LOW)

        def attend(h):
            k_all = kvb[h, 0]
            v_all = kvb[h, 1]
            for g in range(0, group, PACK):
                ats = [pl.ds(pl.multiple_of((h * group + g + n) * hd, hd), hd)
                       for n in range(PACK)]
                q = jnp.concatenate([qbuf[:, at] for at in ats], axis=0)
                s = lax.dot_general(q, k_all, contract_last, preferred_element_type=f32)
                far = jnp.minimum(s[:, :span - tok], cap)
                near = jnp.minimum(s[:, span - tok:], jnp.concatenate([tri[...]] * PACK, axis=0))
                s = jnp.concatenate([far, near], axis=1)
                top = jnp.max(s, axis=1, keepdims=True)
                w = jnp.exp2((s - top) * coef)
                tot = jnp.sum(w, axis=1, keepdims=True)
                o = jnp.dot(w.astype(bf16), v_all, preferred_element_type=f32)
                o = (o * (1.0 / tot)).astype(bf16)
                for n, at in enumerate(ats):
                    out_ref[:, at] = o[n * tok:(n + 1) * tok]

        def combine():
            d_last_in.wait_recv()
            for d in range(n_seq):
                level = jnp.where(diag, dbuf[d // 4, d % 2, d // 2 % 2, heads:heads + 1, :], 0.0)
                lall[d] = jnp.broadcast_to(jnp.sum(level, axis=1, keepdims=True), (heads, hd))
            for p in range(prompts):
                parts = []
                for k in range(reach):
                    d = jnp.minimum(starts[p] + k, n_seq - 1)
                    a, b, c = d // 4, lax.rem(d, 2), lax.rem(d // 2, 2)
                    lse = jnp.where(k < sizes[p], lall[d], LOW)
                    parts.append((lse, a, b, c))
                m = functools.reduce(jnp.maximum, [x[0] for x in parts])
                num = jnp.zeros((heads, hd), f32)
                den = jnp.zeros((heads, hd), f32)
                for lse, a, b, c in parts:
                    w = jnp.exp2(lse - m)
                    den += w
                    num += w * dbuf[a, b, c, 0:heads, :]
                oall[p * heads:(p + 1) * heads, :] = num / den
            for h in range(heads):
                dec_ref[:, h * hd:(h + 1) * hd] = oall[
                    pl.ds(h, prompts, stride=heads), :].astype(bf16)

        far_at = min(2, kvh - 1)
        last_at = min(5, kvh - 1)

        def step(h, carry):
            @pl.when(h + AHEAD < kvh)
            def _():
                each_send(h + AHEAD, start)

            @pl.when(h == far_at)
            def _():
                d_first_in.wait_recv()
                for c in d_far:
                    c.start()

            @pl.when(h == last_at)
            def _():
                for c in d_far_in:
                    c.wait_recv()
                d_last.start()

            @pl.when(h == kvh - 1)
            def _():
                combine()

            @pl.when(h + LEAD < kvh)
            def _():
                each_relay(h + LEAD, start, True)

            each_forward(h, start, True)

            @pl.when(h >= 1)
            def _():
                wait_rest(h - 1)
                attend(h - 1)
            return carry

        for h in range(min(LEAD, kvh)):
            each_relay(h, start, True)
        lax.fori_loop(0, kvh, step, 0)
        wait_rest(kvh - 1)
        attend(kvh - 1)

        d_first.wait_send()
        for c in d_far:
            c.wait_send()
        d_last.wait_send()

        def drain(h, carry):
            each_send(h, wait_send)
            each_near(h, wait_send)
            each_forward(h, wait_send, False)
            each_relay(h, wait_send, False)
            return carry

        lax.fori_loop(0, kvh, drain, 0)

    any_spec = pl.BlockSpec(memory_space=pl.ANY)
    vmem = pl.BlockSpec(memory_space=pltpu.VMEM)
    return pl.pallas_call(
        kernel,
        out_shape=(
            pltpu.VMEM((tok, heads * hd), bf16),
            pltpu.VMEM((prompts, heads * hd), bf16),
        ),
        in_specs=[pl.BlockSpec(memory_space=pltpu.SMEM)] + [any_spec] * 6,
        out_specs=(vmem, vmem),
        scratch_shapes=[
            pltpu.VMEM(new_query.shape, bf16),
            pltpu.VMEM(new_key.shape, bf16),
            pltpu.VMEM(new_value.shape, bf16),
            pltpu.VMEM((tok, heads * hd), bf16),
            pltpu.VMEM((kvh, 2, span, hd), bf16),
            pltpu.VMEM((quads, 2, 2, heads + 8, hd), f32),
            pltpu.VMEM((heads, hd), f32),
            pltpu.VMEM((heads, hd), f32),
            pltpu.VMEM((heads, hd), f32),
            pltpu.VMEM((prompts * heads, hd), f32),
            pltpu.VMEM((n_seq, heads, hd), f32),
            pltpu.VMEM((tok, tok), f32),
            pltpu.SemaphoreType.DMA((kvh, 2)),
            pltpu.SemaphoreType.DMA,
            pltpu.SemaphoreType.DMA((3,)),
            pltpu.SemaphoreType.DMA((kvh, half)),
            pltpu.SemaphoreType.DMA((kvh, half)),
            pltpu.SemaphoreType.DMA((kvh,)),
            pltpu.SemaphoreType.DMA((kvh, reach)),
            pltpu.SemaphoreType.DMA((quads + 1,)),
            pltpu.SemaphoreType.DMA((quads + 1,)),
        ],
        compiler_params=pltpu.CompilerParams(
            collective_id=0, has_side_effects=True, vmem_limit_bytes=56 * 1024 * 1024
        ),
    )(lengths, query, keys, values, new_query, new_key, new_value)


def solution(mesh):
    in_specs = (
        P("groups"),
        P(("groups", "seq"), None),
        P(("groups", "seq"), None),
        P(("groups", "seq"), None),
        P("groups", None),
        P("groups", None),
        P("groups", None),
    )
    out_specs = (P(("groups", "seq"), None), P("groups", None))
    return jax.shard_map(body, mesh=mesh, in_specs=in_specs, out_specs=out_specs, check_vma=False)
```

```python
import functools
import math

import jax
import jax.numpy as jnp
from jax import lax
from jax.experimental import pallas as pl
from jax.experimental.pallas import tpu as pltpu
from jax.sharding import PartitionSpec as P

HEAD_DIM = 128
LOW = -1e30
HIGH = 3e38
AHEAD = 3
LEAD = 2
PACK = 2


def body(lengths, query, keys, values, new_query, new_key, new_value):
    n_seq = lax.axis_size("seq")
    reach = n_seq // 4
    half = reach // 2
    tok = query.shape[0]
    hd = HEAD_DIM
    heads = query.shape[1] // hd
    kvh = keys.shape[1] // hd
    group = heads // kvh
    prompts = new_query.shape[0]
    span = reach * tok
    coef = math.log2(math.e) / math.sqrt(hd)
    quads = n_seq // 4
    f32, bf16 = jnp.float32, jnp.bfloat16

    def kernel(len_ref, q_hbm, k_hbm, v_hbm, nq_hbm, nk_hbm, nv_hbm, out_ref, dec_ref,
               nq_ref, nk_ref, nv_ref, qbuf, kvb, dbuf, qd, nk32, nv32, oall, lall, tri,
               load_sem, q_sem, n_sem, send_sem, fwd_sem, relay_sem, recv_sem, d_send, d_recv):
        me = lax.axis_index("seq")
        core = lax.rem(me, 2)
        sibling = me + 1 - 2 * core

        def load_copies(h):
            return [
                pltpu.make_async_copy(
                    src.at[:, pl.ds(h * hd, hd)],
                    kvb.at[h, part, pl.ds((reach - 1) * tok, tok), :],
                    load_sem.at[h, part],
                )
                for part, src in enumerate((k_hbm, v_hbm))
            ]

        for h in range(kvh):
            for copy in load_copies(h):
                copy.start()
        q_copy = pltpu.make_async_copy(q_hbm, qbuf, q_sem)
        n_copies = [pltpu.make_async_copy(src, dst, n_sem.at[n]) for n, (src, dst) in
                    enumerate(((nq_hbm, nq_ref), (nk_hbm, nk_ref), (nv_hbm, nv_ref)))]
        for copy in n_copies:
            copy.start()
        q_copy.start()

        barrier = pltpu.get_barrier_semaphore()
        for k in range(1, n_seq):
            pl.semaphore_signal(barrier, inc=1, device_id={"seq": lax.rem(me + k, n_seq)},
                                device_id_type=pl.DeviceIdType.MESH)

        run = jnp.int32(0)
        first_dev, pid, is_last = jnp.int32(0), jnp.int32(0), jnp.int32(0)
        starts, sizes = [], []
        for p in range(prompts):
            size = len_ref[p]
            starts.append(run)
            sizes.append(size)
            inside = (run <= me) & (me < run + size)
            first_dev = jnp.where(inside, run, first_dev)
            pid = jnp.where(inside, p, pid)
            is_last = jnp.where(inside & (me == run + size - 1), 1, is_last)
            run = run + size

        pl.semaphore_wait(barrier, n_seq - 1)

        def remote(h, held, put, sem, target):
            return pltpu.make_async_remote_copy(
                src_ref=kvb.at[h, :, pl.ds(held * tok, tok), :],
                dst_ref=kvb.at[h, :, pl.ds(put * tok, tok), :],
                send_sem=sem,
                recv_sem=recv_sem.at[h, put],
                device_id={"seq": target},
                device_id_type=pl.DeviceIdType.MESH,
            )

        own = reach - 1

        odd = lax.rem(me // 2, 2)
        relayed = (core == 1) & (odd == 1) if half == 2 else (core == 2)
        relays = (core == 0) & (odd == 1) & (me >= reach - 1) if half == 2 else (core == 2)

        def each_near(h, act):
            @pl.when(core == 0)
            def _():
                act(remote(h, own, reach - 2, send_sem.at[h, half - 1], me + 1))
            @pl.when((core == 1) & (me + reach - 1 < n_seq))
            def _():
                act(remote(h, own, 0, send_sem.at[h, half - 1], me + reach - 1))

        def each_send(h, act):
            for j in range(1, half):
                @pl.when((me + 2 * j < n_seq) & jnp.logical_not(relayed))
                def _(j=j):
                    act(remote(h, own, own - 2 * j, send_sem.at[h, j - 1], me + 2 * j))

        def each_relay(h, act, arrive):
            if half == 2:
                @pl.when(relays)
                def _():
                    if arrive:
                        remote(h, own, 0, relay_sem.at[h], sibling).wait_recv()
                    act(remote(h, 0, own - 2, relay_sem.at[h], me - 1))

        def each_forward(h, act, arrive):
            for j in range(1, half):
                @pl.when(me >= 2 * j)
                def _(j=j):
                    put = own - 2 * j - 1 + 2 * core
                    copy = remote(h, own - 2 * j, put, fwd_sem.at[h, j - 1], sibling)
                    if arrive:
                        remote(h, own, own - 2 * j, fwd_sem.at[h, j - 1], sibling).wait_recv()
                    act(copy)

        def wait_rest(h):
            for j in range(half):
                here = me >= 2 * j + 1
                if j == half - 1:
                    here = here & jnp.logical_not(relays)
                @pl.when(here)
                def _(j=j):
                    remote(h, own, own - 2 * j - 1, fwd_sem.at[h, 0], sibling).wait_recv()

        start = lambda c: c.start()
        wait_send = lambda c: c.wait_send()
        for h in range(kvh):
            for copy in load_copies(h):
                copy.wait()
            each_near(h, start)
            if h < AHEAD:
                each_send(h, start)

        rows = lax.broadcasted_iota(jnp.int32, (tok, tok), 0)
        cols = lax.broadcasted_iota(jnp.int32, (tok, tok), 1)
        tri[...] = jnp.where(cols <= rows, HIGH, LOW)

        def slot(d):
            return pl.ds((reach - 1 - d) * tok, tok)

        for d in range(1, reach):
            @pl.when(me < d)
            def _(d=d):
                kvb[:, :, slot(d), :] = jnp.zeros((kvh, 2, tok, hd), bf16)

        for copy in n_copies:
            copy.wait()
        picked = lax.broadcasted_iota(jnp.int32, (prompts, hd), 0) == pid

        def pick(ref, h):
            block = ref[:, h * hd:(h + 1) * hd].astype(f32)
            return jnp.sum(jnp.where(picked, block, 0.0), axis=0, keepdims=True)

        for h in range(heads):
            qd[h:h + 1, :] = pick(nq_ref, h)
        for h in range(kvh):
            nk32[h * group:(h + 1) * group, :] = jnp.broadcast_to(pick(nk_ref, h), (group, hd))
            nv32[h * group:(h + 1) * group, :] = jnp.broadcast_to(pick(nv_ref, h), (group, hd))
        q32 = qd[...]
        q32b = q32.astype(bf16)
        row_head = lax.broadcasted_iota(jnp.int32, (heads, tok), 0) // group
        own_rows = pl.ds((reach - 1) * tok, tok)
        contract_last = (((1,), (1,)), ((), ()))
        scores = jnp.zeros((heads, tok), f32)
        for h in range(kvh):
            part = lax.dot_general(q32b, kvb[h, 0, own_rows, :], contract_last,
                                   preferred_element_type=f32)
            scores = jnp.where(row_head == h, part, scores)
        own_score = jnp.sum(q32 * nk32[...], axis=1, keepdims=True)
        own_score = jnp.where(is_last == 1, own_score, LOW)
        peak = jnp.maximum(jnp.max(scores, axis=1, keepdims=True), own_score)
        weights = jnp.exp2((scores - peak) * coef)
        own_weight = jnp.exp2((own_score - peak) * coef)
        total = jnp.sum(weights, axis=1, keepdims=True) + own_weight
        accum = own_weight.astype(bf16).astype(f32) * nv32[...]
        for h in range(kvh):
            masked = jnp.where(row_head == h, weights, 0.0).astype(bf16)
            accum += jnp.dot(masked, kvb[h, 1, own_rows, :], preferred_element_type=f32)

        quad = me // 4
        side = lax.rem(me // 2, 2)
        dbuf[quad, core, side, 0:heads, :] = accum / total
        diag = (lax.broadcasted_iota(jnp.int32, (heads, hd), 0)
                == lax.broadcasted_iota(jnp.int32, (heads, hd), 1))
        level = jnp.where(diag, peak * coef + jnp.log2(total), 0.0)
        dbuf[quad, core, side, heads:, :] = jnp.broadcast_to(
            jnp.sum(level, axis=0, keepdims=True), (8, hd))

        def d_copy(ref, send, recv, target):
            return pltpu.make_async_remote_copy(
                src_ref=ref, dst_ref=ref, send_sem=d_send.at[send], recv_sem=d_recv.at[recv],
                device_id={"seq": target}, device_id_type=pl.DeviceIdType.MESH)

        across = me + 2 - 4 * side
        d_first = d_copy(dbuf.at[quad, core, side], 0, 0, across)
        d_first_in = d_copy(dbuf.at[quad, core, 1 - side], 0, 0, across)
        d_far = [d_copy(dbuf.at[quad, core], k, k, lax.rem(me + 4 * k, n_seq))
                 for k in range(1, quads)]
        d_far_in = [d_copy(dbuf.at[lax.rem(quad + quads - k, quads), core], k, k, sibling)
                    for k in range(1, quads)]
        d_last = d_copy(dbuf.at[:, core], quads, quads, sibling)
        d_last_in = d_copy(dbuf.at[:, 1 - core], quads, quads, sibling)

        d_first.start()
        q_copy.wait()

        block_of = lax.broadcasted_iota(jnp.int32, (1, span - tok), 1) // tok
        cap = jnp.where(me - (reach - 1) + block_of >= first_dev, HIGH, LOW)

        def attend(h):
            k_all = kvb[h, 0]
            v_all = kvb[h, 1]
            v_ones = jnp.concatenate([v_all, jnp.ones_like(v_all)], axis=1)
            for g in range(0, group, PACK):
                ats = [pl.ds(pl.multiple_of((h * group + g + n) * hd, hd), hd)
                       for n in range(PACK)]
                q = jnp.concatenate([qbuf[:, at] for at in ats], axis=0)
                s = lax.dot_general(q, k_all, contract_last, preferred_element_type=f32)
                far = jnp.minimum(s[:, :span - tok], cap)
                near = jnp.minimum(s[:, span - tok:], jnp.concatenate([tri[...]] * PACK, axis=0))
                s = jnp.concatenate([far, near], axis=1)
                top = jnp.max(s, axis=1, keepdims=True)
                w = jnp.exp2((s - top) * coef)
                o = jnp.dot(w.astype(bf16), v_ones, preferred_element_type=f32)
                o = (o[:, :hd] / o[:, hd:]).astype(bf16)
                for n, at in enumerate(ats):
                    out_ref[:, at] = o[n * tok:(n + 1) * tok]

        def combine():
            d_last_in.wait_recv()
            for d in range(n_seq):
                level = jnp.where(diag, dbuf[d // 4, d % 2, d // 2 % 2, heads:heads + 1, :], 0.0)
                lall[d] = jnp.broadcast_to(jnp.sum(level, axis=1, keepdims=True), (heads, hd))
            for p in range(prompts):
                parts = []
                for k in range(reach):
                    d = jnp.minimum(starts[p] + k, n_seq - 1)
                    a, b, c = d // 4, lax.rem(d, 2), lax.rem(d // 2, 2)
                    lse = jnp.where(k < sizes[p], lall[d], LOW)
                    parts.append((lse, a, b, c))
                m = functools.reduce(jnp.maximum, [x[0] for x in parts])
                num = jnp.zeros((heads, hd), f32)
                den = jnp.zeros((heads, hd), f32)
                for lse, a, b, c in parts:
                    w = jnp.exp2(lse - m)
                    den += w
                    num += w * dbuf[a, b, c, 0:heads, :]
                oall[p * heads:(p + 1) * heads, :] = num / den
            for h in range(heads):
                dec_ref[:, h * hd:(h + 1) * hd] = oall[
                    pl.ds(h, prompts, stride=heads), :].astype(bf16)

        far_at = min(2, kvh - 1)
        last_at = min(5, kvh - 1)

        def step(h, carry):
            @pl.when(h + AHEAD < kvh)
            def _():
                each_send(h + AHEAD, start)

            @pl.when(h == far_at)
            def _():
                d_first_in.wait_recv()
                for c in d_far:
                    c.start()

            @pl.when(h == last_at)
            def _():
                for c in d_far_in:
                    c.wait_recv()
                d_last.start()

            @pl.when(h == kvh - 1)
            def _():
                combine()

            @pl.when(h + LEAD < kvh)
            def _():
                each_relay(h + LEAD, start, True)

            each_forward(h, start, True)

            @pl.when(h >= 1)
            def _():
                wait_rest(h - 1)
                attend(h - 1)
            return carry

        for h in range(min(LEAD, kvh)):
            each_relay(h, start, True)
        lax.fori_loop(0, kvh, step, 0)
        wait_rest(kvh - 1)
        attend(kvh - 1)

        d_first.wait_send()
        for c in d_far:
            c.wait_send()
        d_last.wait_send()

        def drain(h, carry):
            each_send(h, wait_send)
            each_near(h, wait_send)
            each_forward(h, wait_send, False)
            each_relay(h, wait_send, False)
            return carry

        lax.fori_loop(0, kvh, drain, 0)

    any_spec = pl.BlockSpec(memory_space=pl.ANY)
    vmem = pl.BlockSpec(memory_space=pltpu.VMEM)
    return pl.pallas_call(
        kernel,
        out_shape=(
            pltpu.VMEM((tok, heads * hd), bf16),
            pltpu.VMEM((prompts, heads * hd), bf16),
        ),
        in_specs=[pl.BlockSpec(memory_space=pltpu.SMEM)] + [any_spec] * 6,
        out_specs=(vmem, vmem),
        scratch_shapes=[
            pltpu.VMEM(new_query.shape, bf16),
            pltpu.VMEM(new_key.shape, bf16),
            pltpu.VMEM(new_value.shape, bf16),
            pltpu.VMEM((tok, heads * hd), bf16),
            pltpu.VMEM((kvh, 2, span, hd), bf16),
            pltpu.VMEM((quads, 2, 2, heads + 8, hd), f32),
            pltpu.VMEM((heads, hd), f32),
            pltpu.VMEM((heads, hd), f32),
            pltpu.VMEM((heads, hd), f32),
            pltpu.VMEM((prompts * heads, hd), f32),
            pltpu.VMEM((n_seq, heads, hd), f32),
            pltpu.VMEM((tok, tok), f32),
            pltpu.SemaphoreType.DMA((kvh, 2)),
            pltpu.SemaphoreType.DMA,
            pltpu.SemaphoreType.DMA((3,)),
            pltpu.SemaphoreType.DMA((kvh, half)),
            pltpu.SemaphoreType.DMA((kvh, half)),
            pltpu.SemaphoreType.DMA((kvh,)),
            pltpu.SemaphoreType.DMA((kvh, reach)),
            pltpu.SemaphoreType.DMA((quads + 1,)),
            pltpu.SemaphoreType.DMA((quads + 1,)),
        ],
        compiler_params=pltpu.CompilerParams(
            collective_id=0, has_side_effects=True, vmem_limit_bytes=56 * 1024 * 1024
        ),
    )(lengths, query, keys, values, new_query, new_key, new_value)


def solution(mesh):
    in_specs = (
        P("groups"),
        P(("groups", "seq"), None),
        P(("groups", "seq"), None),
        P(("groups", "seq"), None),
        P("groups", None),
        P("groups", None),
        P("groups", None),
    )
    out_specs = (P(("groups", "seq"), None), P("groups", None))
    return jax.shard_map(body, mesh=mesh, in_specs=in_specs, out_specs=out_specs, check_vma=False)
```
